32 devices in a mesh: ctx: 16 (over z, x, core), tp: 2 (over y).
Axes of the slice: x: 2, y: 2, z: 4, core: 2. Of those that a mesh axis runs over, the one named last changes fastest.
Arguments:
- queries: bfloat16 [32, 3, 128, 128], P('ctx', None, 'tp'), may hold values from -480 to 480
- prefix_keys: bfloat16 [32768, 8, 128], P('ctx', 'tp'), may hold values from -6 to 6
- prefix_values: bfloat16 [32768, 8, 128], P('ctx', 'tp'), may hold values from -6 to 6
- suffix_keys: bfloat16 [32, 512, 8, 128], P('ctx', None, 'tp'), may hold values from -6 to 6
- suffix_values: bfloat16 [32, 512, 8, 128], P('ctx', None, 'tp'), may hold values from -6 to 6
- fork_lengths: int32 [32], P('ctx'), may hold values from 1 to 509, 8192 in all
- out_weight: bfloat16 [16384, 16384], P('tp', 'ctx'), may hold values from -0.046875 to 0.046875
Outputs:
- projected: bfloat16 [32, 3, 16384], P('tp', None, 'ctx')
The draws below stay inside these ranges and needn't reach their ends.
Inputs may be any that keep to these rules, and one draw needn't show every extreme that they name: `fork_lengths`: A fork's earlier tokens fill the first slots of its suffix, followed by the keys and values of its 3 new tokens.
All inputs are finite; a program needn't handle non-finite values. No bound on the sum of `fork_lengths` on one device may be relied on, other than what follows from the above.
Results may differ from the reference program's by a relative error of at most 0.014.
Values may be sent and summed in bfloat16 or wider, within the bound.
A program may use at most 128 MiB of HBM per device.

```python
import math
import jax
import jax.numpy as jnp
import numpy as np
from jax import lax

D = 16384
HEADS = 128
KV_HEADS = 8
HD = 128
PRE_DEV = 2048
SUF_MAX = 512
STEPS = 3
FORKS = 32
PREFIX = 32768
N_CTX = 16


def draw_queries(key, part):
    shape = (FORKS, STEPS, HEADS, HD)
    base_key = jax.random.fold_in(jax.random.fold_in(key, 11), 0)
    entries = jnp.clip(jax.random.normal(base_key, shape, jnp.float32), -6.0, 6.0)
    return entries.astype(jnp.bfloat16)


def block_levels(key, dims, cuts, least, largest):
    loudness, own = 1.0, jax.random.fold_in(key, 6)
    for axis_at, shards_of in cuts:
        draws = jnp.exp(jax.random.uniform(jax.random.fold_in(own, axis_at), (shards_of,), jnp.float32, least / len(cuts), largest / len(cuts)))
        loudness = loudness * jnp.repeat(draws, dims[axis_at] // shards_of).reshape([-1 if axis == axis_at else 1 for axis in range(len(dims))])
    return loudness


def length_profile(count, total, reach, slope):
    weights = [(1 << 20) // math.isqrt(standing ** slope) + 1 for standing in range(2, count + 1)]
    spare, given = total - reach - (count - 1), [1] * (count - 1)
    while spare > 0:
        candidates = [i for i in range(count - 1) if given[i] < reach]
        pool, left = sum([weights[i] for i in candidates]), spare
        for i in candidates:
            addition = min(reach - given[i], max(1, left * weights[i] // pool), spare)
            given[i] = given[i] + addition
            spare = spare - addition
    return np.array([reach] + given)


def ragged(key, amount, total, bound, slope):
    if amount == 2:
        one = jax.random.randint(key, (), max(1, total - bound), min(bound, total - 1) + 1)
        return jnp.stack([one, total - one])
    lengths = jnp.asarray(length_profile(amount, total, bound, slope), jnp.int32)
    couples = (amount - 1) // 2
    donor, sink = lengths[1:1 + 2 * couples:2], lengths[2:2 + 2 * couples:2]
    margin = jnp.minimum(donor - 1, bound - sink)
    moved = jax.random.randint(jax.random.fold_in(key, 1), (couples,), 0, 1 << 20) % (margin + 1)
    lengths = lengths.at[1:1 + 2 * couples:2].set(donor - moved).at[2:2 + 2 * couples:2].set(sink + moved)
    return lengths[jax.random.permutation(jax.random.fold_in(key, 2), amount)]


def gaussian(own_key, dims, spread, most, cuts=(), kind=jnp.bfloat16):
    factor_of = block_levels(own_key, dims, cuts, -0.22, 0.18) if cuts else 1.0
    values = jax.random.normal(own_key, dims, jnp.float32) * spread * factor_of
    return jnp.minimum(jnp.maximum(values, -most), most).astype(kind)


def setup_inputs(seed: int = 0) -> dict:
    seeds = jax.random.split(jax.random.key(seed), 8)
    queries = draw_queries(jax.random.fold_in(seeds[7], 71), 0)
    prefix_keys = gaussian(seeds[1], (PREFIX, KV_HEADS, HD), 1.0, 6.0, ((0, 16), (1, 2)))
    prefix_values = gaussian(seeds[2], (PREFIX, KV_HEADS, HD), 1.0, 6.0, ((0, 16), (1, 2)))
    suffix_keys = gaussian(seeds[3], (FORKS, SUF_MAX, KV_HEADS, HD), 1.0, 6.0, ((0, 16), (2, 2)))
    suffix_values = gaussian(seeds[4], (FORKS, SUF_MAX, KV_HEADS, HD), 1.0, 6.0, ((0, 16), (2, 2)))
    fork_lengths = ragged(seeds[5], FORKS, FORKS * (SUF_MAX // 2), SUF_MAX - STEPS, 2).astype(jnp.int32)
    out_weight = gaussian(seeds[6], (HEADS * HD, D), (HEADS * HD) ** -0.5, 0.046875, ((0, 2), (1, 16)))
    return dict(queries=queries, prefix_keys=prefix_keys, prefix_values=prefix_values, suffix_keys=suffix_keys, suffix_values=suffix_values, fork_lengths=fork_lengths, out_weight=out_weight)


def combine(first, second):
    mixed_a, highest_a, totals_a = first
    mixed_b, highest_b, totals_b = second
    summit = jnp.maximum(highest_a, highest_b)
    factor_a = jnp.exp(highest_a - summit)
    factor_b = jnp.exp(highest_b - summit)
    mixed = mixed_a * factor_a[..., None] + mixed_b * factor_b[..., None]
    return (mixed, summit, totals_a * factor_a + totals_b * factor_b)


def softmax_state(scores, values, form, shape):
    highest = jnp.max(scores, axis=-1)
    weights = jnp.exp(scores - highest[..., None])
    totals = jnp.sum(weights, axis=-1)
    mixed = jnp.einsum(form, weights.astype(jnp.bfloat16).astype(jnp.float32), values.astype(jnp.float32))
    return (mixed.reshape(shape), highest.reshape(shape[:3]), totals.reshape(shape[:3]))


def reference(queries, prefix_keys, prefix_values, suffix_keys, suffix_values, fork_lengths, out_weight):
    group = HEADS // KV_HEADS
    scale = HD ** -0.5
    width = math.gcd(FORKS, 16)
    blocks = FORKS // width

    def per_block(items):
        block_queries, block_keys, block_values, block_lengths = items
        shape = block_queries.shape
        grouped = block_queries.astype(jnp.float32).reshape(width, STEPS, KV_HEADS, group, HD)
        state = None
        for segment in range(N_CTX):
            seg_keys = prefix_keys[segment * PRE_DEV:(segment + 1) * PRE_DEV].astype(jnp.float32)
            seg_values = prefix_values[segment * PRE_DEV:(segment + 1) * PRE_DEV]
            scores = jnp.einsum("bskgd,pkd->bskgp", grouped, seg_keys) * scale
            partial_state = softmax_state(scores, seg_values, "bskgp,pkd->bskgd", shape)
            state = partial_state if state is None else combine(state, partial_state)
        scores = jnp.einsum("bskgd,bpkd->bskgp", grouped, block_keys.astype(jnp.float32)) * scale
        limit = block_lengths[:, None] + jnp.arange(STEPS, dtype=jnp.int32)[None, :] + 1
        visible = jnp.arange(SUF_MAX, dtype=jnp.int32)[None, None, :] < limit[:, :, None]
        scores = jnp.where(visible[:, :, None, None, :], scores, jnp.float32(-1e30))
        state = combine(state, softmax_state(scores, block_values, "bskgp,bpkd->bskgd", shape))
        mixed, highest, totals = state
        return (mixed / totals[..., None]).astype(jnp.bfloat16)

    attention = lax.map(per_block, (
        queries.reshape(blocks, width, STEPS, HEADS, HD),
        suffix_keys.reshape(blocks, width, SUF_MAX, KV_HEADS, HD),
        suffix_values.reshape(blocks, width, SUF_MAX, KV_HEADS, HD),
        fork_lengths.reshape(blocks, width)))
    rows = attention.reshape(FORKS * STEPS, HEADS * HD)
    result = jnp.dot(rows, out_weight, preferred_element_type=jnp.float32).astype(jnp.bfloat16)
    return result.reshape(FORKS, STEPS, D)
```

```python
import functools
import math

import jax
import jax.numpy as jnp
from jax import lax
from jax.experimental import pallas as pl
from jax.experimental.pallas import tpu as pltpu
from jax.sharding import PartitionSpec as P

MESH = pl.DeviceIdType.MESH
F32 = jnp.float32
BF16 = jnp.bfloat16


def attend(
    n,
    steps,
    lengths_ref,
    q_ref,
    k_ref,
    v_ref,
    sk_ref,
    sv_ref,
    out_ref,
    q_all,
    own,
    own_st,
    psend,
    psend_st,
    precv,
    precv_st,
    csend,
    csend_st,
    crecv,
    crecv_st,
    suf,
    suf_st,
    att,
    qs_sem,
    qr_sem,
    ps_sem,
    pr_sem,
    pss_sem,
    prs_sem,
    cs_sem,
    cr_sem,
    css_sem,
    crs_sem,
    as_sem,
    ar_sem,
):
    kv, rows, hd = q_ref.shape
    forks = sk_ref.shape[0]
    slots = sk_ref.shape[2]
    group = rows // (forks * steps)
    chips = n // 2
    factor = hd ** (-0.5) * math.log2(math.e)
    me = lax.axis_index("ctx")

    def across(mask):
        place, bit = me, 1
        while bit <= mask:
            if mask & bit:
                place = place + bit - 2 * bit * (me // bit % 2)
            bit = 2 * bit
        return place

    barrier = pltpu.get_barrier_semaphore()
    peers = [1] + [2 * chip for chip in range(1, chips)]
    for peer in peers:
        pl.semaphore_signal(
            barrier, inc=1, device_id={"ctx": across(peer)}, device_id_type=MESH
        )
    pl.semaphore_wait(barrier, len(peers))

    def send(source, target, send_sem, recv_sem, peer):
        copy = pltpu.make_async_remote_copy(
            src_ref=source,
            dst_ref=target,
            send_sem=send_sem,
            recv_sem=recv_sem,
            device_id={"ctx": across(peer)},
            device_id_type=MESH,
        )
        copy.start()
        return copy

    class Gather:
        def __init__(self, buf, own_block, send_sems, recv_sems):
            self.buf, self.own_block = buf, own_block
            self.send_sems, self.recv_sems = send_sems, recv_sems
            self.copies = []

        def push(self, slot, peer):
            source = self.own_block if slot == 0 else self.buf.at[slot]
            self.copies.append(
                send(
                    source,
                    self.buf.at[slot ^ peer],
                    self.send_sems.at[len(self.copies)],
                    self.recv_sems.at[slot ^ peer],
                    peer,
                )
            )

        def arrive(self, slot):
            pltpu.make_async_remote_copy(
                src_ref=self.own_block,
                dst_ref=self.buf.at[slot],
                send_sem=self.send_sems.at[0],
                recv_sem=self.recv_sems.at[slot],
                device_id={"ctx": across(1)},
                device_id_type=MESH,
            ).wait_recv()

        def begin(self):
            for chip in range(chips - 2, 0, -2):
                self.push(0, 2 * chip)
            if chips > 1:
                self.push(0, 2)
            self.push(0, 1)

        def near(self):
            self.arrive(2)
            self.push(2, 1)
            self.arrive(1)
            self.arrive(3)

        def far(self):
            for chip in range(2, chips, 2):
                self.arrive(2 * chip)
                self.push(2 * chip, 2)
                self.push(2 * chip, 1)
            for chip in range(3, chips, 2):
                self.arrive(2 * chip)
                self.push(2 * chip, 1)
            for chip in range(2, chips):
                self.arrive(2 * chip + 1)

        def finish(self):
            for copy in self.copies:
                copy.wait_send()

    queries = Gather(q_all, q_ref, qs_sem, qr_sem)
    queries.begin()
    diagonal = lax.broadcasted_iota(jnp.int32, (rows, hd), 0) == lax.broadcasted_iota(
        jnp.int32, (rows, hd), 1
    )

    def to_lanes(column):
        return jnp.sum(
            jnp.where(diagonal, jnp.broadcast_to(column, (rows, hd)), 0.0), axis=0, keepdims=True
        )

    def to_column(lanes):
        return jnp.sum(
            jnp.where(diagonal, jnp.broadcast_to(lanes, (rows, hd)), 0.0), axis=1, keepdims=True
        )

    def state(q, keys, values, visible=None):
        scores = lax.dot_general(
            q, keys, (((1,), (1,)), ((), ())), preferred_element_type=F32
        )
        if visible is not None:
            scores = jnp.where(visible, scores, -1e30)
        highest = jnp.max(scores, axis=1, keepdims=True)
        weights = jnp.exp2((scores - highest) * factor).astype(BF16)
        both = jnp.dot(
            weights,
            jnp.concatenate([values, jnp.ones_like(values)], axis=1),
            preferred_element_type=F32,
        )
        return both[:, :hd], highest * factor, both[:, hd:]

    part = steps * group
    where = lax.broadcasted_iota(jnp.int32, (part, slots), 0) // group
    position = lax.broadcasted_iota(jnp.int32, (part, slots), 1)

    def suffix(head, carry):
        highs, sums = [], []
        for fork in range(forks):
            visible = position < where + (lengths_ref[fork] + 1)
            mixed, high, total = state(
                q_ref[head, pl.ds(fork * part, part), :],
                sk_ref[fork, head],
                sv_ref[fork, head],
                visible,
            )
            suf[head, pl.ds(fork * part, part), :] = mixed
            highs.append(jnp.broadcast_to(high, (part, hd)))
            sums.append(total)
        suf_st[head, 0] = jnp.concatenate(highs, axis=0)
        suf_st[head, 1] = jnp.concatenate(sums, axis=0)
        return carry

    lax.fori_loop(0, kv, suffix, 0)

    def prefix(unit):
        chip = 2 * unit
        places = [2 * chip, 2 * chip + 2, 2 * chip + 1, 2 * chip + 3]

        def one(head, carry):
            q = jnp.concatenate(
                [q_ref[head] if place == 0 else q_all[place, head] for place in places], axis=0
            )
            mixed, high, total = state(q, k_ref[head], v_ref[head])
            for i in range(4):
                block = slice(i * rows, (i + 1) * rows)
                stats, wide = (own_st, own) if i < 2 else (psend_st, psend)
                wide[unit, i % 2, head] = mixed[block].astype(wide.dtype)
                stats[unit, i % 2, pl.ds(2 * head, 1), :] = to_lanes(high[block])
                stats[unit, i % 2, pl.ds(2 * head + 1, 1), :] = to_lanes(total[block])
            return carry

        lax.fori_loop(0, kv, one, 0)
        return (
            send(psend.at[unit], precv.at[unit], ps_sem.at[unit], pr_sem.at[unit], 1),
            send(
                psend_st.at[unit], precv_st.at[unit], pss_sem.at[unit], prs_sem.at[unit], 1
            ),
        )

    outgoing = []

    def pair(unit, copies):
        for copy in copies:
            copy.wait()
        for i in range(2):
            chip = 2 * unit + i
            wide, stats = (csend, csend_st) if chip else (crecv, crecv_st)

            def one(head, carry):
                high_a = own_st[unit, i, pl.ds(2 * head, 1), :]
                high_b = precv_st[unit, i, pl.ds(2 * head, 1), :]
                top = jnp.maximum(high_a, high_b)
                scale_a, scale_b = jnp.exp2(high_a - top), jnp.exp2(high_b - top)
                stats[chip, pl.ds(2 * head, 1), :] = top
                stats[chip, pl.ds(2 * head + 1, 1), :] = (
                    scale_a * own_st[unit, i, pl.ds(2 * head + 1, 1), :]
                    + scale_b * precv_st[unit, i, pl.ds(2 * head + 1, 1), :]
                )
                wide[chip, head] = (
                    own[unit, i, head] * to_column(scale_a)
                    + precv[unit, i, head].astype(F32) * to_column(scale_b)
                ).astype(BF16)
                return carry

            lax.fori_loop(0, kv, one, 0)
            if chip:
                outgoing.append(
                    send(csend.at[chip], crecv.at[chip], cs_sem.at[chip], cr_sem.at[chip], 2 * chip)
                )
                outgoing.append(
                    send(
                        csend_st.at[chip],
                        crecv_st.at[chip],
                        css_sem.at[chip],
                        crs_sem.at[chip],
                        2 * chip,
                    )
                )

    queries.near()
    waiting = (0, prefix(0))
    queries.far()
    for unit in range(chips // 2 - 1, 0, -1):
        copies = prefix(unit)
        pair(*waiting)
        waiting = (unit, copies)
    pair(*waiting)
    queries.finish()
    for copy in outgoing:
        copy.wait()

    def merge(head, carry):
        highs = [crecv_st[chip, pl.ds(2 * head, 1), :] for chip in range(chips)]
        top = functools.reduce(jnp.maximum, highs)
        mixed = jnp.zeros((rows, hd), F32)
        total = jnp.zeros((1, hd), F32)
        for chip in range(chips):
            scale = jnp.exp2(highs[chip] - top)
            total = total + scale * crecv_st[chip, pl.ds(2 * head + 1, 1), :]
            mixed = mixed + crecv[chip, head].astype(F32) * to_column(scale)
        top = to_column(top)
        summit = jnp.maximum(top, suf_st[head, 0])
        scale_a, scale_b = jnp.exp2(top - summit), jnp.exp2(suf_st[head, 0] - summit)
        mixed = mixed * scale_a + suf[head] * scale_b
        total = to_column(total) * scale_a + suf_st[head, 1] * scale_b
        att[0, head] = (mixed / total).astype(BF16)
        return carry

    lax.fori_loop(0, kv, merge, 0)
    attention = Gather(att, att.at[0], as_sem, ar_sem)
    attention.begin()
    attention.near()
    attention.far()
    attention.finish()
    for slot in range(n):
        out_ref[across(slot)] = att[slot]


def shards(
    queries, prefix_keys, prefix_values, suffix_keys, suffix_values, fork_lengths, out_weight
):
    n, tp = lax.axis_size("ctx"), lax.axis_size("tp")
    forks, steps, heads, hd = queries.shape
    kv = prefix_keys.shape[1]
    group = heads // kv
    rows = forks * steps * group
    chips = n // 2
    units = chips // 2
    q = queries.reshape(forks * steps, kv, group, hd).swapaxes(0, 1).reshape(kv, rows, hd)
    vmem = pl.BlockSpec(memory_space=pltpu.VMEM)
    block = (kv, rows, hd)
    stat = (max(8, 2 * kv), hd)
    dma = pltpu.SemaphoreType.DMA
    gathered = pl.pallas_call(
        functools.partial(attend, n, steps),
        out_shape=jax.ShapeDtypeStruct((n,) + block, BF16),
        in_specs=[pl.BlockSpec(memory_space=pltpu.SMEM)] + [vmem] * 5,
        out_specs=vmem,
        scratch_shapes=[
            pltpu.VMEM((n,) + block, BF16),
            pltpu.VMEM((units, 2) + block, F32),
            pltpu.VMEM((units, 2) + stat, F32),
            pltpu.VMEM((units, 2) + block, BF16),
            pltpu.VMEM((units, 2) + stat, F32),
            pltpu.VMEM((units, 2) + block, BF16),
            pltpu.VMEM((units, 2) + stat, F32),
            pltpu.VMEM((chips,) + block, BF16),
            pltpu.VMEM((chips,) + stat, F32),
            pltpu.VMEM((chips,) + block, BF16),
            pltpu.VMEM((chips,) + stat, F32),
            pltpu.VMEM(block, F32),
            pltpu.VMEM((kv, 2, rows, hd), F32),
            pltpu.VMEM((n,) + block, BF16),
            dma((n,)),
            dma((n,)),
            dma((units,)),
            dma((units,)),
            dma((units,)),
            dma((units,)),
            dma((chips,)),
            dma((chips,)),
            dma((chips,)),
            dma((chips,)),
            dma((n,)),
            dma((n,)),
        ],
        compiler_params=pltpu.CompilerParams(
            collective_id=0, has_side_effects=True, vmem_limit_bytes=60 * 1024 * 1024
        ),
    )(
        fork_lengths,
        q,
        prefix_keys.swapaxes(0, 1),
        prefix_values.swapaxes(0, 1),
        suffix_keys.swapaxes(1, 2),
        suffix_values.swapaxes(1, 2),
    )
    attention = (
        gathered.reshape(n, kv, forks * steps, group, hd)
        .transpose(0, 2, 1, 3, 4)
        .reshape(n * forks * steps, heads * hd)
    )
    product = jnp.dot(attention, out_weight, preferred_element_type=F32)
    product = product.reshape(tp, n * forks // tp, steps, -1).astype(BF16)
    mine = lax.axis_index("tp")
    total = lax.dynamic_index_in_dim(product, mine, 0, keepdims=False).astype(F32)
    for shift in range(1, tp):
        piece = lax.dynamic_index_in_dim(product, (mine + shift) % tp, 0, keepdims=False)
        total = total + lax.ppermute(
            piece, "tp", [(i, (i + shift) % tp) for i in range(tp)]
        ).astype(F32)
    return total.astype(BF16)


def solution(mesh):
    return jax.shard_map(
        shards,
        mesh=mesh,
        in_specs=(
            P("ctx", None, "tp", None),
            P("ctx", "tp", None),
            P("ctx", "tp", None),
            P("ctx", None, "tp", None),
            P("ctx", None, "tp", None),
            P("ctx"),
            P("tp", "ctx"),
        ),
        out_specs=P("tp", None, "ctx"),
        check_vma=False,
    )
```

```python
import functools
import math

import jax
import jax.numpy as jnp
from jax import lax
from jax.experimental import pallas as pl
from jax.experimental.pallas import tpu as pltpu
from jax.sharding import PartitionSpec as P

MESH = pl.DeviceIdType.MESH
F32 = jnp.float32
BF16 = jnp.bfloat16


def attend(
    n,
    steps,
    lengths_ref,
    q_ref,
    k_ref,
    v_ref,
    sk_ref,
    sv_ref,
    out_ref,
    q_all,
    own,
    own_st,
    psend,
    psend_st,
    precv,
    precv_st,
    csend,
    csend_st,
    crecv,
    crecv_st,
    suf,
    suf_st,
    att,
    qs_sem,
    qr_sem,
    ps_sem,
    pr_sem,
    pss_sem,
    prs_sem,
    cs_sem,
    cr_sem,
    css_sem,
    crs_sem,
    as_sem,
    ar_sem,
):
    kv, rows, hd = q_ref.shape
    forks = sk_ref.shape[0]
    slots = sk_ref.shape[2]
    group = rows // (forks * steps)
    chips = n // 2
    factor = hd ** (-0.5) * math.log2(math.e)
    me = lax.axis_index("ctx")

    def across(mask):
        place, bit = me, 1
        while bit <= mask:
            if mask & bit:
                place = place + bit - 2 * bit * (me // bit % 2)
            bit = 2 * bit
        return place

    barrier = pltpu.get_barrier_semaphore()
    peers = [1] + [2 * chip for chip in range(1, chips)]
    for peer in peers:
        pl.semaphore_signal(
            barrier, inc=1, device_id={"ctx": across(peer)}, device_id_type=MESH
        )
    pl.semaphore_wait(barrier, len(peers))

    def send(source, target, send_sem, recv_sem, peer):
        copy = pltpu.make_async_remote_copy(
            src_ref=source,
            dst_ref=target,
            send_sem=send_sem,
            recv_sem=recv_sem,
            device_id={"ctx": across(peer)},
            device_id_type=MESH,
        )
        copy.start()
        return copy

    class Gather:
        def __init__(self, buf, own_block, send_sems, recv_sems):
            self.buf, self.own_block = buf, own_block
            self.send_sems, self.recv_sems = send_sems, recv_sems
            self.copies = []

        def push(self, slot, peer):
            source = self.own_block if slot == 0 else self.buf.at[slot]
            self.copies.append(
                send(
                    source,
                    self.buf.at[slot ^ peer],
                    self.send_sems.at[len(self.copies)],
                    self.recv_sems.at[slot ^ peer],
                    peer,
                )
            )

        def arrive(self, slot):
            pltpu.make_async_remote_copy(
                src_ref=self.own_block,
                dst_ref=self.buf.at[slot],
                send_sem=self.send_sems.at[0],
                recv_sem=self.recv_sems.at[slot],
                device_id={"ctx": across(1)},
                device_id_type=MESH,
            ).wait_recv()

        def begin(self):
            for chip in range(chips - 2, 0, -2):
                self.push(0, 2 * chip)
            if chips > 1:
                self.push(0, 2)
            self.push(0, 1)

        def near(self):
            self.arrive(2)
            self.push(2, 1)
            self.arrive(1)
            self.arrive(3)

        def far(self):
            for chip in range(2, chips, 2):
                self.arrive(2 * chip)
                self.push(2 * chip, 2)
                self.push(2 * chip, 1)
            for chip in range(3, chips, 2):
                self.arrive(2 * chip)
                self.push(2 * chip, 1)
            for chip in range(2, chips):
                self.arrive(2 * chip + 1)

        def finish(self):
            for copy in self.copies:
                copy.wait_send()

    queries = Gather(q_all, q_ref, qs_sem, qr_sem)
    queries.begin()
    diagonal = lax.broadcasted_iota(jnp.int32, (rows, hd), 0) == lax.broadcasted_iota(
        jnp.int32, (rows, hd), 1
    )

    def to_lanes(column):
        return jnp.sum(
            jnp.where(diagonal, jnp.broadcast_to(column, (rows, hd)), 0.0), axis=0, keepdims=True
        )

    def to_column(lanes):
        return jnp.sum(
            jnp.where(diagonal, jnp.broadcast_to(lanes, (rows, hd)), 0.0), axis=1, keepdims=True
        )

    def state(q, keys, values, visible=None):
        scores = lax.dot_general(
            q, keys, (((1,), (1,)), ((), ())), preferred_element_type=F32
        )
        if visible is not None:
            scores = jnp.where(visible, scores, -1e30)
        highest = jnp.max(scores, axis=1, keepdims=True)
        weights = jnp.exp2((scores - highest) * factor).astype(BF16)
        both = jnp.dot(
            weights,
            jnp.concatenate([values, jnp.ones_like(values)], axis=1),
            preferred_element_type=F32,
        )
        return both[:, :hd], highest * factor, both[:, hd:]

    part = steps * group
    where = lax.broadcasted_iota(jnp.int32, (part, slots), 0) // group
    position = lax.broadcasted_iota(jnp.int32, (part, slots), 1)

    def suffix(head, carry):
        highs, sums = [], []
        for fork in range(forks):
            visible = position < where + (lengths_ref[fork] + 1)
            mixed, high, total = state(
                q_ref[head, pl.ds(fork * part, part), :],
                sk_ref[fork, head],
                sv_ref[fork, head],
                visible,
            )
            suf[head, pl.ds(fork * part, part), :] = mixed
            highs.append(jnp.broadcast_to(high, (part, hd)))
            sums.append(total)
        suf_st[head, 0] = jnp.concatenate(highs, axis=0)
        suf_st[head, 1] = jnp.concatenate(sums, axis=0)
        return carry

    lax.fori_loop(0, kv, suffix, 0, unroll=True)

    def prefix(unit):
        chip = 2 * unit
        places = [2 * chip, 2 * chip + 2, 2 * chip + 1, 2 * chip + 3]

        def one(head, carry):
            q = jnp.concatenate(
                [q_ref[head] if place == 0 else q_all[place, head] for place in places], axis=0
            )
            mixed, high, total = state(q, k_ref[head], v_ref[head])
            for i in range(4):
                block = slice(i * rows, (i + 1) * rows)
                stats, wide = (own_st, own) if i < 2 else (psend_st, psend)
                wide[unit, i % 2, head] = mixed[block].astype(wide.dtype)
                stats[unit, i % 2, pl.ds(2 * head, 1), :] = to_lanes(high[block])
                stats[unit, i % 2, pl.ds(2 * head + 1, 1), :] = to_lanes(total[block])
            return carry

        lax.fori_loop(0, kv, one, 0, unroll=True)
        return (
            send(psend.at[unit], precv.at[unit], ps_sem.at[unit], pr_sem.at[unit], 1),
            send(
                psend_st.at[unit], precv_st.at[unit], pss_sem.at[unit], prs_sem.at[unit], 1
            ),
        )

    outgoing = []

    def pair(unit, copies):
        for copy in copies:
            copy.wait()
        for i in range(2):
            chip = 2 * unit + i
            wide, stats = (csend, csend_st) if chip else (crecv, crecv_st)

            def one(head, carry):
                high_a = own_st[unit, i, pl.ds(2 * head, 1), :]
                high_b = precv_st[unit, i, pl.ds(2 * head, 1), :]
                top = jnp.maximum(high_a, high_b)
                scale_a, scale_b = jnp.exp2(high_a - top), jnp.exp2(high_b - top)
                stats[chip, pl.ds(2 * head, 1), :] = top
                stats[chip, pl.ds(2 * head + 1, 1), :] = (
                    scale_a * own_st[unit, i, pl.ds(2 * head + 1, 1), :]
                    + scale_b * precv_st[unit, i, pl.ds(2 * head + 1, 1), :]
                )
                wide[chip, head] = (
                    own[unit, i, head] * to_column(scale_a)
                    + precv[unit, i, head].astype(F32) * to_column(scale_b)
                ).astype(BF16)
                return carry

            lax.fori_loop(0, kv, one, 0, unroll=True)
            if chip:
                outgoing.append(
                    send(csend.at[chip], crecv.at[chip], cs_sem.at[chip], cr_sem.at[chip], 2 * chip)
                )
                outgoing.append(
                    send(
                        csend_st.at[chip],
                        crecv_st.at[chip],
                        css_sem.at[chip],
                        crs_sem.at[chip],
                        2 * chip,
                    )
                )

    queries.near()
    waiting = (0, prefix(0))
    queries.far()
    for unit in range(chips // 2 - 1, 0, -1):
        copies = prefix(unit)
        pair(*waiting)
        waiting = (unit, copies)
    pair(*waiting)
    queries.finish()
    for copy in outgoing:
        copy.wait()

    def merge(head, carry):
        highs = [crecv_st[chip, pl.ds(2 * head, 1), :] for chip in range(chips)]
        top = functools.reduce(jnp.maximum, highs)
        mixed = jnp.zeros((rows, hd), F32)
        total = jnp.zeros((1, hd), F32)
        for chip in range(chips):
            scale = jnp.exp2(highs[chip] - top)
            total = total + scale * crecv_st[chip, pl.ds(2 * head + 1, 1), :]
            mixed = mixed + crecv[chip, head].astype(F32) * to_column(scale)
        top = to_column(top)
        summit = jnp.maximum(top, suf_st[head, 0])
        scale_a, scale_b = jnp.exp2(top - summit), jnp.exp2(suf_st[head, 0] - summit)
        mixed = mixed * scale_a + suf[head] * scale_b
        total = to_column(total) * scale_a + suf_st[head, 1] * scale_b
        att[0, head] = (mixed / total).astype(BF16)
        return carry

    lax.fori_loop(0, kv, merge, 0, unroll=True)
    attention = Gather(att, att.at[0], as_sem, ar_sem)
    attention.begin()
    attention.near()
    attention.far()
    attention.finish()
    for slot in range(n):
        out_ref[across(slot)] = att[slot]


def shards(
    queries, prefix_keys, prefix_values, suffix_keys, suffix_values, fork_lengths, out_weight
):
    n, tp = lax.axis_size("ctx"), lax.axis_size("tp")
    forks, steps, heads, hd = queries.shape
    kv = prefix_keys.shape[1]
    group = heads // kv
    rows = forks * steps * group
    chips = n // 2
    units = chips // 2
    q = queries.reshape(forks * steps, kv, group, hd).swapaxes(0, 1).reshape(kv, rows, hd)
    vmem = pl.BlockSpec(memory_space=pltpu.VMEM)
    block = (kv, rows, hd)
    stat = (max(8, 2 * kv), hd)
    dma = pltpu.SemaphoreType.DMA
    gathered = pl.pallas_call(
        functools.partial(attend, n, steps),
        out_shape=jax.ShapeDtypeStruct((n,) + block, BF16),
        in_specs=[pl.BlockSpec(memory_space=pltpu.SMEM)] + [vmem] * 5,
        out_specs=vmem,
        scratch_shapes=[
            pltpu.VMEM((n,) + block, BF16),
            pltpu.VMEM((units, 2) + block, F32),
            pltpu.VMEM((units, 2) + stat, F32),
            pltpu.VMEM((units, 2) + block, BF16),
            pltpu.VMEM((units, 2) + stat, F32),
            pltpu.VMEM((units, 2) + block, BF16),
            pltpu.VMEM((units, 2) + stat, F32),
            pltpu.VMEM((chips,) + block, BF16),
            pltpu.VMEM((chips,) + stat, F32),
            pltpu.VMEM((chips,) + block, BF16),
            pltpu.VMEM((chips,) + stat, F32),
            pltpu.VMEM(block, F32),
            pltpu.VMEM((kv, 2, rows, hd), F32),
            pltpu.VMEM((n,) + block, BF16),
            dma((n,)),
            dma((n,)),
            dma((units,)),
            dma((units,)),
            dma((units,)),
            dma((units,)),
            dma((chips,)),
            dma((chips,)),
            dma((chips,)),
            dma((chips,)),
            dma((n,)),
            dma((n,)),
        ],
        compiler_params=pltpu.CompilerParams(
            collective_id=0, has_side_effects=True, vmem_limit_bytes=60 * 1024 * 1024
        ),
    )(
        fork_lengths,
        q,
        prefix_keys.swapaxes(0, 1),
        prefix_values.swapaxes(0, 1),
        suffix_keys.swapaxes(1, 2),
        suffix_values.swapaxes(1, 2),
    )
    attention = (
        gathered.reshape(n, kv, forks * steps, group, hd)
        .transpose(0, 2, 1, 3, 4)
        .reshape(n * forks * steps, heads * hd)
    )
    product = jnp.dot(attention, out_weight, preferred_element_type=F32)
    product = lax.optimization_barrier(product.astype(BF16))
    product = product.reshape(tp, n * forks // tp, steps, -1)
    mine = lax.axis_index("tp")
    total = lax.dynamic_index_in_dim(product, mine, 0, keepdims=False).astype(F32)
    for shift in range(1, tp):
        piece = lax.dynamic_index_in_dim(product, (mine + shift) % tp, 0, keepdims=False)
        total = total + lax.ppermute(
            piece, "tp", [(i, (i + shift) % tp) for i in range(tp)]
        ).astype(F32)
    return total.astype(BF16)


def solution(mesh):
    return jax.shard_map(
        shards,
        mesh=mesh,
        in_specs=(
            P("ctx", None, "tp", None),
            P("ctx", "tp", None),
            P("ctx", "tp", None),
            P("ctx", None, "tp", None),
            P("ctx", None, "tp", None),
            P("ctx"),
            P("tp", "ctx"),
        ),
        out_specs=P("tp", None, "ctx"),
        check_vma=False,
    )
```
